512 devices in a mesh: batch: 8 (over x, y_lo), seq: 32 (over y_hi, z), section: 2 (over core).
Axes of the slice: x: 4, y: 4 (y_hi: 2, y_lo: 2; y = y_hi * 2 + y_lo), z: 16, core: 2. Of those that a mesh axis runs over, the one named last changes fastest.
Arguments:
- acts: bfloat16 [2, 118784, 5120], P('section', ('batch', 'seq')), may hold values from -13 to 13
- cotangent: float32 [2, 118784, 6], P('section', ('batch', 'seq')), may hold values from -120 to 120
- routes: int32 [2, 118784, 6], P('section', ('batch', 'seq')), may hold values from 0 to 159, all different within a row
- router_weight: bfloat16 [2, 5120, 160], P('section', ('batch', 'seq')), may hold values from -0.078125 to 0.078125
Outputs:
- grad_router: float32 [2, 5120, 160], P('section', ('batch', 'seq'))
The draws below stay inside these ranges and needn't reach their ends.
Inputs may be any that keep to these rules, and one draw needn't show every extreme that they name: `routes`: each token's row names 6 different experts, and every expert is named by some token.
All inputs are finite; a program needn't handle non-finite values.
Results may differ from the reference program's by a relative error of at most 0.0017.
Values may be sent and summed in bfloat16 or wider, within the bound.
No kernel may reach another device: no remote copies, remote signals or barrier semaphores. Data moves between devices by JAX's collectives and lax.ppermute only.
A program may use at most 64 MiB of HBM per device.

```python
import math
import jax
import jax.numpy as jnp
from jax import lax

D = 5120
EXPERTS = 160
TOPK = 6
TOK_DEV = 464
LAYERS = 2
TOKENS = 118784


def draw_acts(key, part):
    groups = TOKENS // TOK_DEV
    block_width = D // groups
    base_key = jax.random.fold_in(key, 11)
    offset_key = jax.random.fold_in(key, 12)
    pair_key = jax.random.fold_in(key, 13)
    base = jnp.clip(jax.random.normal(base_key, (LAYERS, TOKENS, D), jnp.float32), -4.0, 4.0)
    pairing = jax.random.permutation(pair_key, groups)
    token_group = jnp.arange(TOKENS, dtype=jnp.int32) // TOK_DEV
    feature_group = jnp.arange(D, dtype=jnp.int32) // block_width
    paired = pairing[token_group][:, None] == feature_group[None, :]
    spike = jnp.where(paired, 3.0, 1.0).astype(jnp.float32)
    offset = 0.12 * jnp.clip(jax.random.normal(offset_key, (LAYERS, 1, D), jnp.float32), -3.0, 3.0)
    values = base * spike[None, :, :] + offset
    return values.astype(jnp.bfloat16)


def draw_cotangent(key, part):
    base = jnp.clip(jax.random.normal(key, (LAYERS, TOKENS, TOPK), jnp.float32) + 1.5, -4.0, 4.0)
    span = 4.0
    position = jnp.arange(TOKENS, dtype=jnp.float32) / TOKENS
    row_scale = jnp.exp(jnp.log(span) * position)
    layer_scale = 1.0 + 2.0 * jnp.arange(LAYERS, dtype=jnp.float32) / max(LAYERS - 1, 1)
    values = base * row_scale[None, :, None] * layer_scale[:, None, None]
    return values.astype(jnp.float32)


def block_levels(rng, dims, cuts, low, largest):
    factor_of = 1.0
    for dim, parts in cuts:
        heights = jax.random.uniform(jax.random.fold_in(jax.random.fold_in(rng, 6), dim), (parts,), jnp.float32, low / len(cuts), largest / len(cuts))
        factor_of = factor_of * jnp.repeat(jnp.exp(heights), dims[dim] // parts).reshape((-1,) + (1,) * (len(dims) - 1 - dim))
    return factor_of


def different_ones(rng, rows, number_of, top, lift):
    sequence = jax.random.permutation(jax.random.fold_in(rng, 1), number_of)
    favour = sequence
    for power in range(3):
        favour = favour * favour // number_of
    favour = favour * lift // number_of
    chance = jax.random.randint(jax.random.fold_in(rng, 2), (rows, number_of), 0, 4096) + favour
    fixed_rows = jax.random.permutation(jax.random.fold_in(rng, 3), rows)[jnp.arange(number_of) % rows]
    chance = jnp.where(jnp.arange(rows)[:, None] == fixed_rows[None, :], 1 << 14, chance)
    merit = chance * number_of + jnp.arange(number_of)
    return lax.top_k(merit.astype(jnp.int32), top)[1].astype(jnp.int32)


def bell_draw(key, extent, scale, most, pieces=(), held_as=jnp.bfloat16):
    factor_of = block_levels(key, extent, pieces, -0.22, 0.18) if pieces else 1.0
    array = jax.random.normal(key, extent, jnp.float32) * scale * factor_of
    return jnp.minimum(jnp.maximum(array, -most), most).astype(held_as)


def setup_inputs(seed: int = 0) -> dict:
    arg_keys = jax.random.split(jax.random.key(seed), 5)
    return {
        "acts": draw_acts(jax.random.fold_in(arg_keys[4], 71), 0),
        "cotangent": draw_cotangent(jax.random.fold_in(arg_keys[4], 71), 0),
        "routes": different_ones(arg_keys[2], LAYERS * TOKENS, EXPERTS, TOPK, 307).reshape((LAYERS, TOKENS, TOPK)),
        "router_weight": bell_draw(arg_keys[3], (LAYERS, D, EXPERTS), D ** -0.5, 0.078125, ((0, 2), (1, 256))),
    }


def over_tokens(left, right):
    return lax.dot_general(left, right, (((0,), (0,)), ((), ())), preferred_element_type=jnp.float32)

def layer_grad(x_layer, cot_layer, route_layer, weight_layer):
    logits = jnp.dot(x_layer, weight_layer, preferred_element_type=jnp.float32)
    expo = jnp.exp(logits)
    probs = expo / lax.optimization_barrier(jnp.sum(expo, axis=-1, keepdims=True))
    expert_ids = jnp.arange(EXPERTS, dtype=jnp.int32)
    picks = (route_layer[:, :, None] == expert_ids[None, None, :]).astype(jnp.float32)
    d_prob = lax.optimization_barrier(jnp.sum(cot_layer[:, :, None] * picks, axis=1))
    inner = lax.optimization_barrier(jnp.sum(probs * d_prob, axis=-1, keepdims=True))
    d_logits = (probs * (d_prob - inner)).astype(jnp.bfloat16)
    return over_tokens(x_layer, d_logits)

def reference(acts, cotangent, routes, router_weight):
    raw = []
    for layer in range(LAYERS):
        raw.append(layer_grad(acts[layer], cotangent[layer], routes[layer], router_weight[layer]))
    raw = jnp.stack(raw)
    square_sum = jnp.sum(raw * raw)
    clip_norm = 0.25 * math.sqrt(1.0 * LAYERS * D * EXPERTS)
    clip_scale = jnp.minimum(jnp.float32(1.0), clip_norm / jnp.sqrt(square_sum))
    return raw * clip_scale
```

```python
import math

import jax
import jax.numpy as jnp
from jax import lax
from jax.sharding import Mesh
from jax.sharding import PartitionSpec as P

BATCH_SEQ = ("batch_0", "batch_1", "seq_0", "seq_1")
PLANE = ("batch_0", "batch_1", "seq_0")
LINE = ("seq_1",)


def exchanged(parts, axes):
    return lax.all_to_all(parts, axes, split_axis=0, concat_axis=0, tiled=True)


def size(axes):
    return math.prod(lax.axis_size(a) for a in axes)


def gathered(x, axes):
    return exchanged(jnp.broadcast_to(x[None], (size(axes), *x.shape)), axes)


def shards(acts, cotangent, routes, router_weight):
    x = acts[0]
    width = x.shape[1]
    rows, experts = router_weight.shape[1:]
    plane, line = size(PLANE), size(LINE)
    weight = gathered(router_weight.reshape(1, rows * experts), LINE)
    weight = gathered(weight.reshape(-1, 128), PLANE)
    weight = weight.reshape(width, experts)
    logits = jnp.dot(x, weight, preferred_element_type=jnp.float32)
    expo = jnp.exp(logits)
    probs = expo / jnp.sum(expo, axis=-1, keepdims=True)
    expert_ids = jnp.arange(experts, dtype=jnp.int32)
    picks = (routes[0][:, :, None] == expert_ids[None, None, :]).astype(jnp.float32)
    d_prob = jnp.sum(cotangent[0][:, :, None] * picks, axis=1)
    inner = jnp.sum(probs * d_prob, axis=-1, keepdims=True)
    d_logits = (probs * (d_prob - inner)).astype(jnp.bfloat16)
    raw = jnp.einsum("td,te->de", x, d_logits, preferred_element_type=jnp.float32)
    parts = raw.astype(jnp.bfloat16).reshape(plane, -1, 128)
    summed = exchanged(parts, PLANE).astype(jnp.float32).sum(axis=0)
    parts = summed.reshape(line, 1, -1)
    summed = exchanged(parts, LINE).sum(axis=0).reshape(rows, experts)
    squares = jnp.sum(summed * summed)
    for axes in (PLANE, LINE):
        squares = jnp.sum(gathered(jnp.broadcast_to(squares, (1, 128)), axes)[:, 0, 0])
    squares = lax.psum(squares, "section")
    entry_count = 1.0 * lax.axis_size("section") * width * experts
    clip_norm = 0.25 * math.sqrt(entry_count)
    clip_scale = jnp.minimum(jnp.float32(1.0), clip_norm / jnp.sqrt(squares))
    return (summed * clip_scale)[None]


def solution(mesh):
    torus = Mesh(
        mesh.devices.reshape(4, 2, 2, 16, mesh.shape["section"]),
        ("batch_0", "batch_1", "seq_0", "seq_1", "section"),
    )
    placed = P("section", BATCH_SEQ, None)
    return jax.shard_map(
        shards,
        mesh=torus,
        in_specs=(placed, placed, placed, placed),
        out_specs=placed,
        check_vma=False,
    )
```

```python
import functools
import math

import jax
import jax.numpy as jnp
from jax import lax
from jax.experimental import pallas as pl
from jax.experimental.pallas import tpu as pltpu
from jax.sharding import Mesh
from jax.sharding import PartitionSpec as P

BATCH_SEQ = ("batch_0", "batch_1", "seq_0", "seq_1")
PLANE = ("batch_0", "batch_1", "seq_0")
LINE = ("seq_1",)

F32, BF16, I16, I32 = jnp.float32, jnp.bfloat16, jnp.int16, jnp.int32
LANES = 128
WIDE = 160
REST = WIDE - LANES
FOLD = LANES // REST
TOP = 32700.0


def exchanged(parts, axes):
    return lax.all_to_all(parts, axes, split_axis=0, concat_axis=0, tiled=True)


def size(axes):
    return math.prod(lax.axis_size(a) for a in axes)


def exponent_of(biggest):
    return jnp.floor(jnp.log2(TOP / jnp.maximum(biggest, 1e-30)))


def folded(block):
    step = block.shape[0] // FOLD
    rest = [block[step * g : step * (g + 1), LANES:WIDE] for g in range(FOLD)]
    return block[:, :LANES], jnp.concatenate(rest, axis=1)


def spread_kernel(w_ref, out_ref):
    wide, rest = folded(w_ref[...].astype(F32))
    piece = jnp.concatenate([wide, rest], axis=0).astype(BF16)
    out_ref[...] = jnp.broadcast_to(piece[None], out_ref.shape)


def chunk_kernel(rows, p_ref, out_ref, wide, rest):
    pieces = p_ref.shape[0]
    step = rows // FOLD
    group = pieces // FOLD
    for c in range(pieces):
        piece = p_ref[c].astype(F32)
        wide[rows * c : rows * (c + 1), :] = piece[:rows]
        k = c // group
        for g in range(FOLD):
            row = rows * (c % group) + step * g
            rest[row : row + step, REST * k : REST * (k + 1)] = piece[
                rows : rows + step, REST * g : REST * (g + 1)
            ]
    deep = wide.shape[0]
    full = deep + rest.shape[0]
    out_ref[:, :deep, :] = jnp.broadcast_to(
        wide[...].astype(BF16)[None], (out_ref.shape[0], deep, LANES)
    )
    out_ref[:, deep:full, :] = jnp.broadcast_to(
        rest[...].astype(BF16)[None], (out_ref.shape[0], full - deep, LANES)
    )


def layer_kernel(x_hbm, w_ref, c_ref, r_ref, out_ref, x, weight, logits, sems):
    tokens, width = x.shape
    chunks = w_ref.shape[0]
    deep = width // chunks
    block = deep // FOLD
    pairs = chunks // 2
    cols = width // pairs
    copies = [
        pltpu.make_async_copy(
            x_hbm.at[:, cols * j : cols * (j + 1)],
            x.at[:, cols * j : cols * (j + 1)],
            sems.at[j],
        )
        for j in range(pairs)
    ]
    for copy in copies:
        copy.start()
    for g in range(chunks):
        weight[deep * g : deep * (g + 1), :LANES] = w_ref[g, :deep, :]
        rest = w_ref[g, deep : deep + block, :].astype(F32)
        for k in range(FOLD):
            turned = rest if k == 0 else pltpu.roll(rest, LANES - REST * k, axis=1)
            row = deep * g + block * k
            weight[row : row + block, LANES:] = turned.astype(BF16)
    logits[tokens:, :] = jnp.zeros((logits.shape[0] - tokens, logits.shape[1]), F32)
    total = None
    for j in range(pairs):
        copies[j].wait()
        part = jnp.dot(
            x[:, cols * j : cols * (j + 1)],
            weight[cols * j : cols * (j + 1), :],
            preferred_element_type=F32,
        )
        total = part if total is None else total + part
    logits[:tokens, :] = total
    flipped = jnp.transpose(logits[...])[:WIDE, :tokens]
    expo = jnp.exp(flipped)
    probs = expo / jnp.sum(expo, axis=0, keepdims=True)
    expert = lax.broadcasted_iota(I32, (WIDE, tokens), 0)
    d_prob = jnp.zeros((WIDE, tokens), F32)
    for k in range(c_ref.shape[0]):
        d_prob = d_prob + jnp.where(expert == r_ref[k], c_ref[k], 0.0)
    inner = jnp.sum(probs * d_prob, axis=0, keepdims=True)
    d_logits = (probs * (d_prob - inner)).astype(BF16)

    half = WIDE // 2
    left = lax.broadcasted_iota(I32, (WIDE, LANES), 1) < LANES // 2
    row16 = lax.broadcasted_iota(I32, (16, LANES), 0)

    def coded(tile):
        k = exponent_of(jnp.max(jnp.abs(tile), axis=0, keepdims=True))
        return jnp.round(tile * jnp.exp2(k)).astype(I32).astype(I16), k

    def pair(j):
        raw = jnp.dot(d_logits, x[:, cols * j : cols * (j + 1)], preferred_element_type=F32)
        tiles = [raw[:, LANES * i : LANES * (i + 1)] for i in range(5)]
        turned = [None, None] + [pltpu.roll(t, LANES // 2, axis=1) for t in tiles[2:]]
        for odd, (one, two, low, high) in enumerate(
            (
                (tiles[0], tiles[1], tiles[2], turned[2]),
                (
                    jnp.where(left, turned[2], turned[3]),
                    jnp.where(left, turned[3], turned[4]),
                    turned[4],
                    tiles[4],
                ),
            )
        ):
            three = jnp.where(left[:half], low[:half], high[half:])
            one, one_k = coded(one)
            two, two_k = coded(two)
            three, three_k = coded(three)
            g = 2 * j + odd
            out_ref[g, 0:WIDE, :] = one
            out_ref[g, WIDE : 2 * WIDE, :] = two
            out_ref[g, 2 * WIDE : 2 * WIDE + half, :] = three
            keys = jnp.where(row16 == 0, one_k, jnp.where(row16 == 1, two_k, three_k))
            out_ref[g, 2 * WIDE + half :, :] = keys.astype(I32).astype(I16)

    for j in range(pairs):
        pair(j)


def plane_sum_kernel(rows, q_ref, out_ref, table):
    half = WIDE // 2
    base = 2 * WIDE + half
    one = jnp.zeros((WIDE, LANES), F32)
    two = jnp.zeros((WIDE, LANES), F32)
    three = jnp.zeros((half, LANES), F32)
    for s in range(q_ref.shape[0]):
        keys = jnp.exp2(-q_ref[s, base:, :].astype(I32).astype(F32))
        one = one + q_ref[s, :WIDE, :].astype(I32).astype(F32) * keys[0:1]
        two = two + q_ref[s, WIDE : 2 * WIDE, :].astype(I32).astype(F32) * keys[1:2]
        three = three + q_ref[s, 2 * WIDE : base, :].astype(I32).astype(F32) * keys[2:3]
    table[0:LANES, :WIDE] = jnp.transpose(one)
    table[LANES : 2 * LANES, :WIDE] = jnp.transpose(two)
    three = jnp.transpose(three)
    mid = LANES // 2
    table[2 * LANES : 2 * LANES + mid, :WIDE] = jnp.concatenate(
        [three[:mid], three[mid:]], axis=1
    )
    for c in range(out_ref.shape[0]):
        block = table[rows * c : rows * (c + 1), :WIDE]
        k = exponent_of(jnp.max(jnp.abs(block), axis=(0, 1), keepdims=True))
        wide, rest = folded(jnp.round(block * jnp.exp2(k)))
        tail = out_ref.shape[1] - rows - rest.shape[0]
        piece = jnp.concatenate([wide, rest, jnp.broadcast_to(k, (tail, LANES))], axis=0)
        out_ref[c] = piece.astype(I32).astype(I16)


def line_sum_kernel(q_ref, raw_ref, square_ref):
    deep = raw_ref.shape[0]
    raw = jnp.zeros(raw_ref.shape, F32)
    for s in range(q_ref.shape[0]):
        piece = q_ref[s].astype(I32).astype(F32)
        raw = raw + piece[:deep] * jnp.exp2(-piece[deep : deep + 1])
    raw_ref[...] = raw
    square = jnp.sum(raw * raw, axis=(0, 1), keepdims=True)
    square_ref[...] = jnp.broadcast_to(square[None], square_ref.shape)


def again_kernel(s_ref, out_ref):
    out_ref[...] = jnp.broadcast_to(jnp.sum(s_ref[...], axis=0, keepdims=True), out_ref.shape)


def clip_kernel(clip_norm, s_ref, raw_ref, out_ref):
    square = jnp.sum(s_ref[...], axis=0)[:, :1]
    scale = jnp.minimum(1.0, clip_norm / jnp.sqrt(square))
    out = raw_ref[...] * scale
    rows = out_ref.shape[0]
    step = rows // FOLD
    out_ref[:, :LANES] = out[:rows]
    for g in range(FOLD):
        out_ref[step * g : step * (g + 1), LANES:] = out[rows:, REST * g : REST * (g + 1)]


def call(kernel, *args, out, scratch=(), specs=None, name=None):
    vmem = pl.BlockSpec(memory_space=pltpu.VMEM)
    many = isinstance(out, list)
    return pl.pallas_call(
        kernel,
        out_shape=out,
        in_specs=specs or [vmem] * len(args),
        out_specs=[vmem] * len(out) if many else vmem,
        scratch_shapes=list(scratch),
        name=name,
    )(*args)


def shards(acts, cotangent, routes, router_weight):
    tokens, width = acts.shape[1:]
    rows, experts = router_weight.shape[1:]
    plane, line = size(PLANE), size(LINE)
    section = lax.axis_size("section")
    deep = rows * line
    fold_rows = rows + rows // FOLD
    fold_deep = deep + deep // FOLD
    like = jax.ShapeDtypeStruct

    weight = call(
        spread_kernel, router_weight[0], out=like((line, fold_rows, LANES), BF16), name="spread"
    )
    weight = exchanged(weight, LINE)
    weight = call(
        functools.partial(chunk_kernel, rows),
        weight,
        out=like((plane, fold_deep, LANES), BF16),
        scratch=[pltpu.VMEM((deep, LANES), F32), pltpu.VMEM((deep // FOLD, LANES), F32)],
        name="chunk",
    )
    weight = exchanged(weight, PLANE)
    vmem = pl.BlockSpec(memory_space=pltpu.VMEM)
    parts = call(
        layer_kernel,
        acts[0],
        weight,
        jnp.transpose(cotangent, (2, 0, 1)),
        jnp.transpose(routes, (2, 0, 1)),
        specs=[pl.BlockSpec(memory_space=pl.ANY), vmem, vmem, vmem],
        out=like((plane, fold_deep + 16, LANES), I16),
        scratch=[
            pltpu.VMEM((tokens, width), BF16),
            pltpu.VMEM((width, 2 * LANES), BF16),
            pltpu.VMEM((-(-tokens // LANES) * LANES, 2 * LANES), F32),
            pltpu.SemaphoreType.DMA((plane // 2,)),
        ],
        name="layer",
    )
    parts = exchanged(parts, PLANE)
    parts = call(
        functools.partial(plane_sum_kernel, rows),
        parts,
        out=like((line, 32, LANES), I16),
        scratch=[pltpu.VMEM((deep, 2 * LANES), F32)],
        name="plane_sum",
    )
    parts = exchanged(parts, LINE)
    raw, square = call(
        line_sum_kernel,
        parts,
        out=[like((fold_rows, LANES), F32), like((plane * section, 1, LANES), F32)],
        name="line_sum",
    )
    square = exchanged(square, (*PLANE, "section"))
    square = call(again_kernel, square, out=like((line, 1, LANES), F32), name="again")
    square = exchanged(square, LINE)
    clip_norm = 0.25 * math.sqrt(1.0 * section * width * experts)
    out = call(
        functools.partial(clip_kernel, clip_norm),
        square,
        raw,
        out=like((rows, experts), F32),
        name="clip",
    )
    return out[None]


def solution(mesh):
    torus = Mesh(
        mesh.devices.reshape(4, 2, 2, 16, mesh.shape["section"]),
        ("batch_0", "batch_1", "seq_0", "seq_1", "section"),
    )
    placed = P("section", BATCH_SEQ, None)
    return jax.shard_map(
        shards,
        mesh=torus,
        in_specs=(placed, placed, placed, placed),
        out_specs=placed,
        check_vma=False,
    )
```

```python
import functools
import math

import jax
import jax.numpy as jnp
from jax import lax
from jax.experimental import pallas as pl
from jax.experimental.pallas import tpu as pltpu
from jax.sharding import Mesh
from jax.sharding import PartitionSpec as P

BATCH_SEQ = ("batch_0", "batch_1", "seq_0", "seq_1")
PLANE = ("batch_0", "batch_1", "seq_0")
LINE = ("seq_1",)

F32, BF16, I16, I32 = jnp.float32, jnp.bfloat16, jnp.int16, jnp.int32
LANES = 128
WIDE = 160
REST = WIDE - LANES
FOLD = LANES // REST
TOP = 32700.0


def exchanged(parts, axes):
    return lax.all_to_all(parts, axes, split_axis=0, concat_axis=0, tiled=True)


def size(axes):
    return math.prod(lax.axis_size(a) for a in axes)


def exponent_of(biggest):
    return jnp.floor(jnp.log2(TOP / jnp.maximum(biggest, 1e-30)))


def folded(block):
    step = block.shape[0] // FOLD
    rest = [block[step * g : step * (g + 1), LANES:WIDE] for g in range(FOLD)]
    return block[:, :LANES], jnp.concatenate(rest, axis=1)


def spread_kernel(w_ref, out_ref):
    wide, rest = folded(w_ref[...].astype(F32))
    piece = jnp.concatenate([wide, rest], axis=0).astype(BF16)
    out_ref[...] = jnp.broadcast_to(piece[None], out_ref.shape)


def chunk_kernel(rows, p_ref, out_ref, wide, rest):
    pieces = p_ref.shape[0]
    step = rows // FOLD
    group = pieces // FOLD
    for c in range(pieces):
        piece = p_ref[c].astype(F32)
        wide[rows * c : rows * (c + 1), :] = piece[:rows]
        k = c // group
        for g in range(FOLD):
            row = rows * (c % group) + step * g
            rest[row : row + step, REST * k : REST * (k + 1)] = piece[
                rows : rows + step, REST * g : REST * (g + 1)
            ]
    deep = wide.shape[0]
    full = deep + rest.shape[0]
    out_ref[:, :deep, :] = jnp.broadcast_to(
        wide[...].astype(BF16)[None], (out_ref.shape[0], deep, LANES)
    )
    out_ref[:, deep:full, :] = jnp.broadcast_to(
        rest[...].astype(BF16)[None], (out_ref.shape[0], full - deep, LANES)
    )


def layer_kernel(x, w_ref, c_ref, r_ref, out_ref, weight, logits):
    tokens, width = x.shape
    chunks = w_ref.shape[0]
    deep = width // chunks
    block = deep // FOLD
    pairs = chunks // 2
    cols = width // pairs
    for g in range(chunks):
        weight[deep * g : deep * (g + 1), :LANES] = w_ref[g, :deep, :]
        rest = w_ref[g, deep : deep + block, :].astype(F32)
        for k in range(FOLD):
            turned = rest if k == 0 else pltpu.roll(rest, LANES - REST * k, axis=1)
            row = deep * g + block * k
            weight[row : row + block, LANES:] = turned.astype(BF16)
    logits[tokens:, :] = jnp.zeros((logits.shape[0] - tokens, logits.shape[1]), F32)
    total = None
    for j in range(pairs):
        part = jnp.dot(
            x[:, cols * j : cols * (j + 1)],
            weight[cols * j : cols * (j + 1), :],
            preferred_element_type=F32,
        )
        total = part if total is None else total + part
    logits[:tokens, :] = total
    flipped = jnp.transpose(logits[...])[:WIDE, :tokens]
    expo = jnp.exp(flipped)
    probs = expo / jnp.sum(expo, axis=0, keepdims=True)
    expert = lax.broadcasted_iota(I32, (WIDE, tokens), 0)
    d_prob = jnp.zeros((WIDE, tokens), F32)
    for k in range(c_ref.shape[0]):
        d_prob = d_prob + jnp.where(expert == r_ref[k], c_ref[k], 0.0)
    inner = jnp.sum(probs * d_prob, axis=0, keepdims=True)
    d_logits = (probs * (d_prob - inner)).astype(BF16)

    half = WIDE // 2
    left = lax.broadcasted_iota(I32, (WIDE, LANES), 1) < LANES // 2
    row16 = lax.broadcasted_iota(I32, (16, LANES), 0)

    def coded(tile):
        k = exponent_of(jnp.max(jnp.abs(tile), axis=0, keepdims=True))
        return jnp.round(tile * jnp.exp2(k)).astype(I32).astype(I16), k

    def pair(j):
        raw = jnp.dot(d_logits, x[:, cols * j : cols * (j + 1)], preferred_element_type=F32)
        tiles = [raw[:, LANES * i : LANES * (i + 1)] for i in range(5)]
        turned = [None, None] + [pltpu.roll(t, LANES // 2, axis=1) for t in tiles[2:]]
        for odd, (one, two, low, high) in enumerate(
            (
                (tiles[0], tiles[1], tiles[2], turned[2]),
                (
                    jnp.where(left, turned[2], turned[3]),
                    jnp.where(left, turned[3], turned[4]),
                    turned[4],
                    tiles[4],
                ),
            )
        ):
            three = jnp.where(left[:half], low[:half], high[half:])
            one, one_k = coded(one)
            two, two_k = coded(two)
            three, three_k = coded(three)
            g = 2 * j + odd
            out_ref[g, 0:WIDE, :] = one
            out_ref[g, WIDE : 2 * WIDE, :] = two
            out_ref[g, 2 * WIDE : 2 * WIDE + half, :] = three
            keys = jnp.where(row16 == 0, one_k, jnp.where(row16 == 1, two_k, three_k))
            out_ref[g, 2 * WIDE + half :, :] = keys.astype(I32).astype(I16)

    for j in range(pairs):
        pair(j)


def plane_sum_kernel(rows, q_ref, out_ref, table):
    half = WIDE // 2
    base = 2 * WIDE + half
    one = jnp.zeros((WIDE, LANES), F32)
    two = jnp.zeros((WIDE, LANES), F32)
    three = jnp.zeros((half, LANES), F32)
    for s in range(q_ref.shape[0]):
        keys = jnp.exp2(-q_ref[s, base:, :].astype(I32).astype(F32))
        one = one + q_ref[s, :WIDE, :].astype(I32).astype(F32) * keys[0:1]
        two = two + q_ref[s, WIDE : 2 * WIDE, :].astype(I32).astype(F32) * keys[1:2]
        three = three + q_ref[s, 2 * WIDE : base, :].astype(I32).astype(F32) * keys[2:3]
    table[0:LANES, :WIDE] = jnp.transpose(one)
    table[LANES : 2 * LANES, :WIDE] = jnp.transpose(two)
    three = jnp.transpose(three)
    mid = LANES // 2
    table[2 * LANES : 2 * LANES + mid, :WIDE] = jnp.concatenate(
        [three[:mid], three[mid:]], axis=1
    )
    for c in range(out_ref.shape[0]):
        block = table[rows * c : rows * (c + 1), :WIDE]
        k = exponent_of(jnp.max(jnp.abs(block), axis=(0, 1), keepdims=True))
        wide, rest = folded(jnp.round(block * jnp.exp2(k)))
        tail = out_ref.shape[1] - rows - rest.shape[0]
        piece = jnp.concatenate([wide, rest, jnp.broadcast_to(k, (tail, LANES))], axis=0)
        out_ref[c] = piece.astype(I32).astype(I16)


def line_sum_kernel(q_ref, raw_ref, square_ref):
    deep = raw_ref.shape[0]
    raw = jnp.zeros(raw_ref.shape, F32)
    for s in range(q_ref.shape[0]):
        piece = q_ref[s].astype(I32).astype(F32)
        raw = raw + piece[:deep] * jnp.exp2(-piece[deep : deep + 1])
    raw_ref[...] = raw
    square = jnp.sum(raw * raw, axis=(0, 1), keepdims=True)
    square_ref[...] = jnp.broadcast_to(square[None], square_ref.shape)


def again_kernel(s_ref, out_ref):
    out_ref[...] = jnp.broadcast_to(jnp.sum(s_ref[...], axis=0, keepdims=True), out_ref.shape)


def clip_kernel(clip_norm, s_ref, raw_ref, out_ref):
    square = jnp.sum(s_ref[...], axis=0)[:, :1]
    scale = jnp.minimum(1.0, clip_norm / jnp.sqrt(square))
    out = raw_ref[...] * scale
    rows = out_ref.shape[0]
    step = rows // FOLD
    out_ref[:, 0, :LANES] = out[:rows]
    for g in range(FOLD):
        out_ref[step * g : step * (g + 1), 0, LANES:] = out[rows:, REST * g : REST * (g + 1)]


def call(kernel, *args, out, mib, scratch=(), name=None):
    vmem = pl.BlockSpec(memory_space=pltpu.VMEM)
    many = isinstance(out, list)
    return pl.pallas_call(
        kernel,
        out_shape=out,
        in_specs=[vmem] * len(args),
        out_specs=[vmem] * len(out) if many else vmem,
        scratch_shapes=list(scratch),
        compiler_params=pltpu.CompilerParams(vmem_limit_bytes=mib << 20),
        name=name,
    )(*args)


def shards(acts, cotangent, routes, router_weight):
    tokens, width = acts.shape[1:]
    rows, experts = router_weight.shape[1:]
    plane, line = size(PLANE), size(LINE)
    section = lax.axis_size("section")
    deep = rows * line
    fold_rows = rows + rows // FOLD
    fold_deep = deep + deep // FOLD
    like = jax.ShapeDtypeStruct

    weight = call(
        spread_kernel, router_weight[0], out=like((line, fold_rows, LANES), BF16), mib=2, name="spread"
    )
    weight = exchanged(weight, LINE)
    weight = call(
        functools.partial(chunk_kernel, rows),
        weight,
        out=like((plane, fold_deep, LANES), BF16),
        scratch=[pltpu.VMEM((deep, LANES), F32), pltpu.VMEM((deep // FOLD, LANES), F32)],
        mib=4, name="chunk",
    )
    weight = exchanged(weight, PLANE)
    parts = call(
        layer_kernel,
        acts[0],
        weight,
        jnp.transpose(cotangent, (2, 0, 1)),
        jnp.transpose(routes, (2, 0, 1)),
        out=like((plane, fold_deep + 16, LANES), I16),
        scratch=[
            pltpu.VMEM((width, 2 * LANES), BF16),
            pltpu.VMEM((-(-tokens // LANES) * LANES, 2 * LANES), F32),
        ],
        mib=20, name="layer",
    )
    parts = exchanged(parts, PLANE)
    parts = call(
        functools.partial(plane_sum_kernel, rows),
        parts,
        out=like((line, 32, LANES), I16),
        scratch=[pltpu.VMEM((deep, 2 * LANES), F32)],
        mib=6, name="plane_sum",
    )
    parts = exchanged(parts, LINE)
    raw, square = call(
        line_sum_kernel,
        parts,
        out=[like((fold_rows, LANES), F32), like((plane * section, 1, LANES), F32)],
        mib=2, name="line_sum",
    )
    square = exchanged(square, (*PLANE, "section"))
    square = call(again_kernel, square, out=like((line, 1, LANES), F32), mib=1, name="again")
    square = exchanged(square, LINE)
    clip_norm = 0.25 * math.sqrt(1.0 * section * width * experts)
    out = call(
        functools.partial(clip_kernel, clip_norm),
        square,
        raw,
        out=like((rows, 1, experts), F32),
        mib=1, name="clip",
    )
    return jnp.transpose(out, (1, 0, 2))


def solution(mesh):
    torus = Mesh(
        mesh.devices.reshape(4, 2, 2, 16, mesh.shape["section"]),
        ("batch_0", "batch_1", "seq_0", "seq_1", "section"),
    )
    placed = P("section", BATCH_SEQ, None)
    return jax.shard_map(
        shards,
        mesh=torus,
        in_specs=(placed, placed, placed, placed),
        out_specs=placed,
        check_vma=False,
    )
```

```python
import functools
import math

import jax
import jax.numpy as jnp
import numpy as np
from jax import lax
from jax.experimental import pallas as pl
from jax.experimental.pallas import tpu as pltpu
from jax.sharding import Mesh
from jax.sharding import PartitionSpec as P

BATCH_SEQ = ("batch_0", "batch_1", "seq_0", "seq_1")
PLANE = ("batch_0", "batch_1", "seq_0")
LINE = ("seq_1",)
EVERY = BATCH_SEQ + ("section",)

F32, BF16, I16, I32 = jnp.float32, jnp.bfloat16, jnp.int16, jnp.int32
LANES = 128
WIDE = 160
REST = WIDE - LANES
FOLD = LANES // REST
TOP = 32700.0
LAG = 13000


def size(axes):
    return math.prod(lax.axis_size(a) for a in axes)


def ids():
    sizes = [lax.axis_size(a) for a in EVERY]
    index = np.arange(math.prod(sizes)).reshape(sizes)
    for axis, name in enumerate(EVERY):
        if name != "batch_1":
            index = np.roll(index, -(sizes[axis] // 2), axis=axis)
    return index.reshape(size(PLANE), size(LINE), 2)


def plane_order():
    row, near, far = (lax.axis_size(a) for a in PLANE)
    index = np.arange(row * near * far).reshape(row, near, far)
    return np.roll(index, (-(row // 2), -(far // 2)), axis=(0, 2)).ravel().tolist()


def line_order():
    line = size(LINE)
    return np.roll(np.arange(line), -(line // 2)).tolist()


def exchanged(parts, groups):
    return lax.all_to_all(
        parts, EVERY, split_axis=0, concat_axis=0, axis_index_groups=groups.tolist(), tiled=True
    )


def over_plane(parts):
    return exchanged(parts, np.moveaxis(ids(), 0, -1).reshape(-1, size(PLANE)))


def over_line(parts):
    return exchanged(parts, np.moveaxis(ids(), 1, -1).reshape(-1, size(LINE)))


def over_plane_and_section(parts):
    return exchanged(parts, ids().transpose(1, 2, 0).reshape(size(LINE), -1))


def exponent_of(biggest):
    return jnp.floor(jnp.log2(TOP / jnp.maximum(biggest, 1e-30)))


def folded(block):
    step = block.shape[0] // FOLD
    rest = [block[step * g : step * (g + 1), LANES:WIDE] for g in range(FOLD)]
    return block[:, :LANES], jnp.concatenate(rest, axis=1)


def spread_kernel(w_ref, out_ref):
    @pl.when(lax.axis_index("section") == 1)
    def _():
        pl.delay(LAG)

    wide, rest = folded(w_ref[...].astype(F32))
    piece = jnp.concatenate([wide, rest], axis=0).astype(BF16)
    out_ref[...] = jnp.broadcast_to(piece[None], out_ref.shape)


def chunk_kernel(rows, order, p_ref, out_ref, wide, rest):
    pieces = p_ref.shape[0]
    step = rows // FOLD
    group = pieces // FOLD
    for c in range(pieces):
        piece = p_ref[order.index(c)].astype(F32)
        wide[rows * c : rows * (c + 1), :] = piece[:rows]
        k = c // group
        for g in range(FOLD):
            row = rows * (c % group) + step * g
            rest[row : row + step, REST * k : REST * (k + 1)] = piece[
                rows : rows + step, REST * g : REST * (g + 1)
            ]
    deep = wide.shape[0]
    full = deep + rest.shape[0]
    out_ref[:, :deep, :] = jnp.broadcast_to(
        wide[...].astype(BF16)[None], (out_ref.shape[0], deep, LANES)
    )
    out_ref[:, deep:full, :] = jnp.broadcast_to(
        rest[...].astype(BF16)[None], (out_ref.shape[0], full - deep, LANES)
    )


def layer_kernel(order, x, w_ref, c_ref, r_ref, out_ref, weight, logits):
    tokens, width = x.shape
    chunks = w_ref.shape[0]
    deep = width // chunks
    block = deep // FOLD
    pairs = chunks // 2
    cols = width // pairs
    for g in range(chunks):
        weight[deep * g : deep * (g + 1), :LANES] = w_ref[order.index(g), :deep, :]
        rest = w_ref[order.index(g), deep : deep + block, :].astype(F32)
        for k in range(FOLD):
            turned = rest if k == 0 else pltpu.roll(rest, LANES - REST * k, axis=1)
            row = deep * g + block * k
            weight[row : row + block, LANES:] = turned.astype(BF16)
    logits[tokens:, :] = jnp.zeros((logits.shape[0] - tokens, logits.shape[1]), F32)
    total = None
    for j in range(pairs):
        part = jnp.dot(
            x[:, cols * j : cols * (j + 1)],
            weight[cols * j : cols * (j + 1), :],
            preferred_element_type=F32,
        )
        total = part if total is None else total + part
    logits[:tokens, :] = total
    flipped = jnp.transpose(logits[...])[:WIDE, :tokens]
    expo = jnp.exp(flipped)
    probs = expo / jnp.sum(expo, axis=0, keepdims=True)
    expert = lax.broadcasted_iota(I32, (WIDE, tokens), 0)
    d_prob = jnp.zeros((WIDE, tokens), F32)
    for k in range(c_ref.shape[0]):
        d_prob = d_prob + jnp.where(expert == r_ref[k], c_ref[k], 0.0)
    inner = jnp.sum(probs * d_prob, axis=0, keepdims=True)
    d_logits = (probs * (d_prob - inner)).astype(BF16)

    half = WIDE // 2
    left = lax.broadcasted_iota(I32, (WIDE, LANES), 1) < LANES // 2
    row16 = lax.broadcasted_iota(I32, (16, LANES), 0)

    def coded(tile):
        k = exponent_of(jnp.max(jnp.abs(tile), axis=0, keepdims=True))
        return jnp.round(tile * jnp.exp2(k)).astype(I32).astype(I16), k

    def pair(j):
        raw = jnp.dot(d_logits, x[:, cols * j : cols * (j + 1)], preferred_element_type=F32)
        tiles = [raw[:, LANES * i : LANES * (i + 1)] for i in range(5)]
        turned = [None, None] + [pltpu.roll(t, LANES // 2, axis=1) for t in tiles[2:]]
        for odd, (one, two, low, high) in enumerate(
            (
                (tiles[0], tiles[1], tiles[2], turned[2]),
                (
                    jnp.where(left, turned[2], turned[3]),
                    jnp.where(left, turned[3], turned[4]),
                    turned[4],
                    tiles[4],
                ),
            )
        ):
            three = jnp.where(left[:half], low[:half], high[half:])
            one, one_k = coded(one)
            two, two_k = coded(two)
            three, three_k = coded(three)
            g = order.index(2 * j + odd)
            out_ref[g, 0:WIDE, :] = one
            out_ref[g, WIDE : 2 * WIDE, :] = two
            out_ref[g, 2 * WIDE : 2 * WIDE + half, :] = three
            keys = jnp.where(row16 == 0, one_k, jnp.where(row16 == 1, two_k, three_k))
            out_ref[g, 2 * WIDE + half :, :] = keys.astype(I32).astype(I16)

    for j in range(pairs):
        pair(j)


def plane_sum_kernel(rows, order, q_ref, out_ref, table):
    half = WIDE // 2
    base = 2 * WIDE + half
    one = jnp.zeros((WIDE, LANES), F32)
    two = jnp.zeros((WIDE, LANES), F32)
    three = jnp.zeros((half, LANES), F32)
    for s in range(q_ref.shape[0]):
        keys = jnp.exp2(-q_ref[s, base:, :].astype(I32).astype(F32))
        one = one + q_ref[s, :WIDE, :].astype(I32).astype(F32) * keys[0:1]
        two = two + q_ref[s, WIDE : 2 * WIDE, :].astype(I32).astype(F32) * keys[1:2]
        three = three + q_ref[s, 2 * WIDE : base, :].astype(I32).astype(F32) * keys[2:3]
    table[0:LANES, :WIDE] = jnp.transpose(one)
    table[LANES : 2 * LANES, :WIDE] = jnp.transpose(two)
    three = jnp.transpose(three)
    mid = LANES // 2
    table[2 * LANES : 2 * LANES + mid, :WIDE] = jnp.concatenate(
        [three[:mid], three[mid:]], axis=1
    )
    for c in range(out_ref.shape[0]):
        block = table[rows * c : rows * (c + 1), :WIDE]
        k = exponent_of(jnp.max(jnp.abs(block), axis=(0, 1), keepdims=True))
        wide, rest = folded(jnp.round(block * jnp.exp2(k)))
        tail = out_ref.shape[1] - rows - rest.shape[0]
        piece = jnp.concatenate([wide, rest, jnp.broadcast_to(k, (tail, LANES))], axis=0)
        out_ref[order.index(c)] = piece.astype(I32).astype(I16)


def line_sum_kernel(q_ref, raw_ref, square_ref):
    deep = raw_ref.shape[0]
    raw = jnp.zeros(raw_ref.shape, F32)
    for s in range(q_ref.shape[0]):
        piece = q_ref[s].astype(I32).astype(F32)
        raw = raw + piece[:deep] * jnp.exp2(-piece[deep : deep + 1])
    raw_ref[...] = raw
    square = jnp.sum(raw * raw, axis=(0, 1), keepdims=True)
    square_ref[...] = jnp.broadcast_to(square[None], square_ref.shape)


def again_kernel(s_ref, out_ref):
    out_ref[...] = jnp.broadcast_to(jnp.sum(s_ref[...], axis=0, keepdims=True), out_ref.shape)


def clip_kernel(clip_norm, s_ref, raw_ref, out_ref):
    square = jnp.sum(s_ref[...], axis=0)[:, :1]
    scale = jnp.minimum(1.0, clip_norm / jnp.sqrt(square))
    out = raw_ref[...] * scale
    rows = out_ref.shape[0]
    step = rows // FOLD
    out_ref[:, 0, :LANES] = out[:rows]
    for g in range(FOLD):
        out_ref[step * g : step * (g + 1), 0, LANES:] = out[rows:, REST * g : REST * (g + 1)]


def call(kernel, *args, out, mib, scratch=(), name=None):
    vmem = pl.BlockSpec(memory_space=pltpu.VMEM)
    many = isinstance(out, list)
    return pl.pallas_call(
        kernel,
        out_shape=out,
        in_specs=[vmem] * len(args),
        out_specs=[vmem] * len(out) if many else vmem,
        scratch_shapes=list(scratch),
        compiler_params=pltpu.CompilerParams(vmem_limit_bytes=mib << 20),
        name=name,
    )(*args)


def shards(acts, cotangent, routes, router_weight):
    tokens, width = acts.shape[1:]
    rows, experts = router_weight.shape[1:]
    plane, line = size(PLANE), size(LINE)
    section = lax.axis_size("section")
    deep = rows * line
    fold_rows = rows + rows // FOLD
    fold_deep = deep + deep // FOLD
    like = jax.ShapeDtypeStruct

    weight = call(
        spread_kernel, router_weight[0], out=like((line, fold_rows, LANES), BF16), mib=2, name="spread"
    )
    weight = over_line(weight)
    weight = call(
        functools.partial(chunk_kernel, rows, line_order()),
        weight,
        out=like((plane, fold_deep, LANES), BF16),
        scratch=[pltpu.VMEM((deep, LANES), F32), pltpu.VMEM((deep // FOLD, LANES), F32)],
        mib=4, name="chunk",
    )
    weight = over_plane(weight)
    parts = call(
        functools.partial(layer_kernel, plane_order()),
        acts[0],
        weight,
        jnp.transpose(cotangent, (2, 0, 1)),
        jnp.transpose(routes, (2, 0, 1)),
        out=like((plane, fold_deep + 16, LANES), I16),
        scratch=[
            pltpu.VMEM((width, 2 * LANES), BF16),
            pltpu.VMEM((-(-tokens // LANES) * LANES, 2 * LANES), F32),
        ],
        mib=20, name="layer",
    )
    parts = over_plane(parts)
    parts = call(
        functools.partial(plane_sum_kernel, rows, line_order()),
        parts,
        out=like((line, 32, LANES), I16),
        scratch=[pltpu.VMEM((deep, 2 * LANES), F32)],
        mib=6, name="plane_sum",
    )
    parts = over_line(parts)
    raw, square = call(
        line_sum_kernel,
        parts,
        out=[like((fold_rows, LANES), F32), like((plane * section, 1, LANES), F32)],
        mib=2, name="line_sum",
    )
    square = over_plane_and_section(square)
    square = call(again_kernel, square, out=like((line, 1, LANES), F32), mib=1, name="again")
    square = over_line(square)
    clip_norm = 0.25 * math.sqrt(1.0 * section * width * experts)
    out = call(
        functools.partial(clip_kernel, clip_norm),
        square,
        raw,
        out=like((rows, 1, experts), F32),
        mib=1, name="clip",
    )
    return jnp.transpose(out, (1, 0, 2))


def solution(mesh):
    torus = Mesh(
        mesh.devices.reshape(4, 2, 2, 16, mesh.shape["section"]),
        ("batch_0", "batch_1", "seq_0", "seq_1", "section"),
    )
    placed = P("section", BATCH_SEQ, None)
    return jax.shard_map(
        shards,
        mesh=torus,
        in_specs=(placed, placed, placed, placed),
        out_specs=placed,
        check_vma=False,
    )
```

```python
import functools
import math

import jax
import jax.numpy as jnp
import numpy as np
from jax import lax
from jax.experimental import pallas as pl
from jax.experimental.pallas import tpu as pltpu
from jax.sharding import Mesh
from jax.sharding import PartitionSpec as P

BATCH_SEQ = ("batch_0", "batch_1", "seq_0", "seq_1")
PLANE = ("batch_0", "batch_1", "seq_0")
LINE = ("seq_1",)
EVERY = BATCH_SEQ + ("section",)

F32, BF16, I16, I32 = jnp.float32, jnp.bfloat16, jnp.int16, jnp.int32
LANES = 128
WIDE = 160
REST = WIDE - LANES
FOLD = LANES // REST
TOP = 32700.0
LAG = 6500


def size(axes):
    return math.prod(lax.axis_size(a) for a in axes)


def ids():
    sizes = [lax.axis_size(a) for a in EVERY]
    index = np.arange(math.prod(sizes)).reshape(sizes)
    for axis, name in enumerate(EVERY):
        if name != "batch_1":
            index = np.roll(index, -(sizes[axis] // 2), axis=axis)
    return index.reshape(size(PLANE), size(LINE), 2)


def plane_order():
    row, near, far = (lax.axis_size(a) for a in PLANE)
    index = np.arange(row * near * far).reshape(row, near, far)
    return np.roll(index, (-(row // 2), -(far // 2)), axis=(0, 2)).ravel().tolist()


def line_order():
    line = size(LINE)
    return np.roll(np.arange(line), -(line // 2)).tolist()


def exchanged(parts, groups):
    return lax.all_to_all(
        parts, EVERY, split_axis=0, concat_axis=0, axis_index_groups=groups.tolist(), tiled=True
    )


def over_plane(parts):
    return exchanged(parts, np.moveaxis(ids(), 0, -1).reshape(-1, size(PLANE)))


def over_line(parts):
    return exchanged(parts, np.moveaxis(ids(), 1, -1).reshape(-1, size(LINE)))


def over_plane_and_section(parts):
    return exchanged(parts, ids().transpose(1, 2, 0).reshape(size(LINE), -1))


def exponent_of(biggest):
    return jnp.floor(jnp.log2(TOP / jnp.maximum(biggest, 1e-30)))


def folded(block):
    step = block.shape[0] // FOLD
    rest = [block[step * g : step * (g + 1), LANES:WIDE] for g in range(FOLD)]
    return block[:, :LANES], jnp.concatenate(rest, axis=1)


def spread_kernel(w_ref, out_ref):
    @pl.when(lax.axis_index("section") == 0)
    def _():
        pl.delay(LAG)

    wide, rest = folded(w_ref[...].astype(F32))
    piece = jnp.concatenate([wide, rest], axis=0).astype(BF16)
    out_ref[...] = jnp.broadcast_to(piece[None], out_ref.shape)


def chunk_kernel(rows, order, p_ref, out_ref, wide, rest):
    pieces = p_ref.shape[0]
    step = rows // FOLD
    group = pieces // FOLD
    for c in range(pieces):
        piece = p_ref[order.index(c)].astype(F32)
        wide[rows * c : rows * (c + 1), :] = piece[:rows]
        k = c // group
        for g in range(FOLD):
            row = rows * (c % group) + step * g
            rest[row : row + step, REST * k : REST * (k + 1)] = piece[
                rows : rows + step, REST * g : REST * (g + 1)
            ]
    deep = wide.shape[0]
    full = deep + rest.shape[0]
    out_ref[:, :deep, :] = jnp.broadcast_to(
        wide[...].astype(BF16)[None], (out_ref.shape[0], deep, LANES)
    )
    out_ref[:, deep:full, :] = jnp.broadcast_to(
        rest[...].astype(BF16)[None], (out_ref.shape[0], full - deep, LANES)
    )


def layer_kernel(order, x, w_ref, c_ref, r_ref, out_ref, weight, logits):
    tokens, width = x.shape
    chunks = w_ref.shape[0]
    deep = width // chunks
    block = deep // FOLD
    pairs = chunks // 2
    cols = width // pairs
    for g in range(chunks):
        weight[deep * g : deep * (g + 1), :LANES] = w_ref[order.index(g), :deep, :]
        rest = w_ref[order.index(g), deep : deep + block, :].astype(F32)
        for k in range(FOLD):
            turned = rest if k == 0 else pltpu.roll(rest, LANES - REST * k, axis=1)
            row = deep * g + block * k
            weight[row : row + block, LANES:] = turned.astype(BF16)
    logits[tokens:, :] = jnp.zeros((logits.shape[0] - tokens, logits.shape[1]), F32)
    total = jnp.dot(x[...], weight[...], preferred_element_type=F32)
    logits[:tokens, :] = total
    flipped = jnp.transpose(logits[...])[:WIDE, :tokens]
    expo = jnp.exp(flipped)
    probs = expo / jnp.sum(expo, axis=0, keepdims=True)
    expert = lax.broadcasted_iota(I32, (WIDE, tokens), 0)
    d_prob = jnp.zeros((WIDE, tokens), F32)
    for k in range(c_ref.shape[0]):
        d_prob = d_prob + jnp.where(expert == r_ref[k], c_ref[k], 0.0)
    inner = jnp.sum(probs * d_prob, axis=0, keepdims=True)
    d_logits = (probs * (d_prob - inner)).astype(BF16)

    half = WIDE // 2
    left = lax.broadcasted_iota(I32, (WIDE, LANES), 1) < LANES // 2
    row16 = lax.broadcasted_iota(I32, (16, LANES), 0)

    def coded(tile):
        k = exponent_of(jnp.max(jnp.abs(tile), axis=0, keepdims=True))
        return jnp.round(tile * jnp.exp2(k)).astype(I32).astype(I16), k

    def pair(j):
        raw = jnp.dot(d_logits, x[:, cols * j : cols * (j + 1)], preferred_element_type=F32)
        tiles = [raw[:, LANES * i : LANES * (i + 1)] for i in range(5)]
        turned = [None, None] + [pltpu.roll(t, LANES // 2, axis=1) for t in tiles[2:]]
        for odd, (one, two, low, high) in enumerate(
            (
                (tiles[0], tiles[1], tiles[2], turned[2]),
                (
                    jnp.where(left, turned[2], turned[3]),
                    jnp.where(left, turned[3], turned[4]),
                    turned[4],
                    tiles[4],
                ),
            )
        ):
            three = jnp.where(left[:half], low[:half], high[half:])
            one, one_k = coded(one)
            two, two_k = coded(two)
            three, three_k = coded(three)
            g = order.index(2 * j + odd)
            out_ref[g, 0:WIDE, :] = one
            out_ref[g, WIDE : 2 * WIDE, :] = two
            out_ref[g, 2 * WIDE : 2 * WIDE + half, :] = three
            keys = jnp.where(row16 == 0, one_k, jnp.where(row16 == 1, two_k, three_k))
            out_ref[g, 2 * WIDE + half :, :] = keys.astype(I32).astype(I16)

    for j in range(pairs):
        pair(j)


def plane_sum_kernel(rows, order, q_ref, out_ref, table):
    half = WIDE // 2
    base = 2 * WIDE + half
    one = jnp.zeros((WIDE, LANES), F32)
    two = jnp.zeros((WIDE, LANES), F32)
    three = jnp.zeros((half, LANES), F32)
    for s in range(q_ref.shape[0]):
        keys = jnp.exp2(-q_ref[s, base:, :].astype(I32).astype(F32))
        one = one + q_ref[s, :WIDE, :].astype(I32).astype(F32) * keys[0:1]
        two = two + q_ref[s, WIDE : 2 * WIDE, :].astype(I32).astype(F32) * keys[1:2]
        three = three + q_ref[s, 2 * WIDE : base, :].astype(I32).astype(F32) * keys[2:3]
    table[0:LANES, :WIDE] = jnp.transpose(one)
    table[LANES : 2 * LANES, :WIDE] = jnp.transpose(two)
    three = jnp.transpose(three)
    mid = LANES // 2
    table[2 * LANES : 2 * LANES + mid, :WIDE] = jnp.concatenate(
        [three[:mid], three[mid:]], axis=1
    )
    for c in range(out_ref.shape[0]):
        block = table[rows * c : rows * (c + 1), :WIDE]
        k = exponent_of(jnp.max(jnp.abs(block), axis=(0, 1), keepdims=True))
        wide, rest = folded(jnp.round(block * jnp.exp2(k)))
        tail = out_ref.shape[1] - rows - rest.shape[0]
        piece = jnp.concatenate([wide, rest, jnp.broadcast_to(k, (tail, LANES))], axis=0)
        out_ref[order.index(c)] = piece.astype(I32).astype(I16)


def line_sum_kernel(q_ref, raw_ref, square_ref):
    deep = raw_ref.shape[0]
    raw = jnp.zeros(raw_ref.shape, F32)
    for s in range(q_ref.shape[0]):
        piece = q_ref[s].astype(I32).astype(F32)
        raw = raw + piece[:deep] * jnp.exp2(-piece[deep : deep + 1])
    raw_ref[...] = raw
    square = jnp.sum(raw * raw, axis=(0, 1), keepdims=True)
    square_ref[...] = jnp.broadcast_to(square[None], square_ref.shape)


def again_kernel(s_ref, out_ref):
    out_ref[...] = jnp.broadcast_to(jnp.sum(s_ref[...], axis=0, keepdims=True), out_ref.shape)


def clip_kernel(clip_norm, s_ref, raw_ref, out_ref):
    square = jnp.sum(s_ref[...], axis=0)[:, :1]
    scale = jnp.minimum(1.0, clip_norm / jnp.sqrt(square))
    out = raw_ref[...] * scale
    rows = out_ref.shape[0]
    step = rows // FOLD
    out_ref[:, 0, :LANES] = out[:rows]
    for g in range(FOLD):
        out_ref[step * g : step * (g + 1), 0, LANES:] = out[rows:, REST * g : REST * (g + 1)]


def call(kernel, *args, out, mib, scratch=(), name=None):
    vmem = pl.BlockSpec(memory_space=pltpu.VMEM)
    many = isinstance(out, list)
    return pl.pallas_call(
        kernel,
        out_shape=out,
        in_specs=[vmem] * len(args),
        out_specs=[vmem] * len(out) if many else vmem,
        scratch_shapes=list(scratch),
        compiler_params=pltpu.CompilerParams(vmem_limit_bytes=mib << 20),
        name=name,
    )(*args)


def shards(acts, cotangent, routes, router_weight):
    tokens, width = acts.shape[1:]
    rows, experts = router_weight.shape[1:]
    plane, line = size(PLANE), size(LINE)
    section = lax.axis_size("section")
    deep = rows * line
    fold_rows = rows + rows // FOLD
    fold_deep = deep + deep // FOLD
    like = jax.ShapeDtypeStruct

    weight = call(
        spread_kernel, router_weight[0], out=like((line, fold_rows, LANES), BF16), mib=2, name="spread"
    )
    weight = over_line(weight)
    weight = call(
        functools.partial(chunk_kernel, rows, line_order()),
        weight,
        out=like((plane, fold_deep, LANES), BF16),
        scratch=[pltpu.VMEM((deep, LANES), F32), pltpu.VMEM((deep // FOLD, LANES), F32)],
        mib=4, name="chunk",
    )
    weight = over_plane(weight)
    parts = call(
        functools.partial(layer_kernel, plane_order()),
        acts[0],
        weight,
        jnp.transpose(cotangent, (2, 0, 1)),
        jnp.transpose(routes, (2, 0, 1)),
        out=like((plane, fold_deep + 16, LANES), I16),
        scratch=[
            pltpu.VMEM((width, 2 * LANES), BF16),
            pltpu.VMEM((-(-tokens // LANES) * LANES, 2 * LANES), F32),
        ],
        mib=20, name="layer",
    )
    parts = over_plane(parts)
    parts = call(
        functools.partial(plane_sum_kernel, rows, line_order()),
        parts,
        out=like((line, 32, LANES), I16),
        scratch=[pltpu.VMEM((deep, 2 * LANES), F32)],
        mib=6, name="plane_sum",
    )
    parts = over_line(parts)
    raw, square = call(
        line_sum_kernel,
        parts,
        out=[like((fold_rows, LANES), F32), like((plane * section, 1, LANES), F32)],
        mib=2, name="line_sum",
    )
    square = over_plane_and_section(square)
    square = call(again_kernel, square, out=like((line, 1, LANES), F32), mib=1, name="again")
    square = over_line(square)
    clip_norm = 0.25 * math.sqrt(1.0 * section * width * experts)
    out = call(
        functools.partial(clip_kernel, clip_norm),
        square,
        raw,
        out=like((rows, 1, experts), F32),
        mib=1, name="clip",
    )
    return jnp.transpose(out, (1, 0, 2))


def solution(mesh):
    torus = Mesh(
        mesh.devices.reshape(4, 2, 2, 16, mesh.shape["section"]),
        ("batch_0", "batch_1", "seq_0", "seq_1", "section"),
    )
    placed = P("section", BATCH_SEQ, None)
    return jax.shard_map(
        shards,
        mesh=torus,
        in_specs=(placed, placed, placed, placed),
        out_specs=placed,
        check_vma=False,
    )
```

```python
import functools
import math

import jax
import jax.numpy as jnp
import numpy as np
from jax import lax
from jax.experimental import pallas as pl
from jax.experimental.pallas import tpu as pltpu
from jax.sharding import Mesh
from jax.sharding import PartitionSpec as P

BATCH_SEQ = ("batch_0", "batch_1", "seq_0", "seq_1")
PLANE = ("batch_0", "batch_1", "seq_0")
LINE = ("seq_1",)
EVERY = BATCH_SEQ + ("section",)

F32, BF16, I16, I32 = jnp.float32, jnp.bfloat16, jnp.int16, jnp.int32
LANES = 128
WIDE = 160
REST = WIDE - LANES
FOLD = LANES // REST
TOP = 32700.0
LAG = 6500


def size(axes):
    return math.prod(lax.axis_size(a) for a in axes)


def ids():
    sizes = [lax.axis_size(a) for a in EVERY]
    index = np.arange(math.prod(sizes)).reshape(sizes)
    for axis, name in enumerate(EVERY):
        if name != "batch_1":
            index = np.roll(index, -(sizes[axis] // 2), axis=axis)
    return index.reshape(size(PLANE), size(LINE), 2)


def plane_order():
    row, near, far = (lax.axis_size(a) for a in PLANE)
    index = np.arange(row * near * far).reshape(row, near, far)
    return np.roll(index, (-(row // 2), -(far // 2)), axis=(0, 2)).ravel().tolist()


def line_order():
    line = size(LINE)
    return np.roll(np.arange(line), -(line // 2)).tolist()


def exchanged(parts, groups):
    return lax.all_to_all(
        parts, EVERY, split_axis=0, concat_axis=0, axis_index_groups=groups.tolist(), tiled=True
    )


def over_plane(parts):
    return exchanged(parts, np.moveaxis(ids(), 0, -1).reshape(-1, size(PLANE)))


def over_line(parts):
    return exchanged(parts, np.moveaxis(ids(), 1, -1).reshape(-1, size(LINE)))


def over_plane_and_section(parts):
    return exchanged(parts, ids().transpose(1, 2, 0).reshape(size(LINE), -1))


def exponent_of(biggest):
    return jnp.floor(jnp.log2(TOP / jnp.maximum(biggest, 1e-30)))


def folded(block):
    step = block.shape[0] // FOLD
    rest = [block[step * g : step * (g + 1), LANES:WIDE] for g in range(FOLD)]
    return block[:, :LANES], jnp.concatenate(rest, axis=1)


def spread_kernel(w_ref, out_ref):
    @pl.when(lax.axis_index("section") == 0)
    def _():
        pl.delay(LAG)

    wide, rest = folded(w_ref[...].astype(F32))
    piece = jnp.concatenate([wide, rest], axis=0).astype(BF16)
    out_ref[...] = jnp.broadcast_to(piece[None], out_ref.shape)


def chunk_kernel(rows, order, p_ref, out_ref, wide, rest):
    pieces = p_ref.shape[0]
    step = rows // FOLD
    group = pieces // FOLD
    for c in range(pieces):
        piece = p_ref[order.index(c)].astype(F32)
        wide[rows * c : rows * (c + 1), :] = piece[:rows]
        k = c // group
        for g in range(FOLD):
            row = rows * (c % group) + step * g
            rest[row : row + step, REST * k : REST * (k + 1)] = piece[
                rows : rows + step, REST * g : REST * (g + 1)
            ]
    deep = wide.shape[0]
    full = deep + rest.shape[0]
    out_ref[:, :deep, :] = jnp.broadcast_to(
        wide[...].astype(BF16)[None], (out_ref.shape[0], deep, LANES)
    )
    out_ref[:, deep:full, :] = jnp.broadcast_to(
        rest[...].astype(BF16)[None], (out_ref.shape[0], full - deep, LANES)
    )


def layer_kernel(order, x, w_ref, c_ref, r_ref, out_ref, weight, logits):
    tokens, width = x.shape
    chunks = w_ref.shape[0]
    deep = width // chunks
    block = deep // FOLD
    pairs = chunks // 2
    cols = width // pairs
    for g in range(chunks):
        weight[deep * g : deep * (g + 1), :LANES] = w_ref[order.index(g), :deep, :]
        rest = w_ref[order.index(g), deep : deep + block, :].astype(F32)
        for k in range(FOLD):
            turned = rest if k == 0 else pltpu.roll(rest, LANES - REST * k, axis=1)
            row = deep * g + block * k
            weight[row : row + block, LANES:] = turned.astype(BF16)
    logits[tokens:, :] = jnp.zeros((logits.shape[0] - tokens, logits.shape[1]), F32)
    total = jnp.dot(x[...], weight[...], preferred_element_type=F32)
    logits[:tokens, :] = total
    flipped = jnp.transpose(logits[...])[:WIDE, :tokens]
    expo = jnp.exp(flipped)
    probs = expo / jnp.sum(expo, axis=0, keepdims=True)
    expert = lax.broadcasted_iota(I32, (WIDE, tokens), 0)
    d_prob = jnp.zeros((WIDE, tokens), F32)
    for k in range(c_ref.shape[0]):
        d_prob = d_prob + jnp.where(expert == r_ref[k], c_ref[k], 0.0)
    inner = jnp.sum(probs * d_prob, axis=0, keepdims=True)
    d_logits = (probs * (d_prob - inner)).astype(BF16)

    half = WIDE // 2
    left = lax.broadcasted_iota(I32, (WIDE, LANES), 1) < LANES // 2
    row8 = lax.broadcasted_iota(I32, (8, LANES), 0)

    def coded(tile):
        k = exponent_of(jnp.max(jnp.abs(tile), axis=0, keepdims=True))
        return jnp.round(tile * jnp.exp2(k)).astype(I32).astype(I16), k

    def pair(j):
        raw = jnp.dot(d_logits, x[:, cols * j : cols * (j + 1)], preferred_element_type=F32)
        tiles = [raw[:, LANES * i : LANES * (i + 1)] for i in range(5)]
        turned = [None, None] + [pltpu.roll(t, LANES // 2, axis=1) for t in tiles[2:]]
        for odd, (one, two, low, high) in enumerate(
            (
                (tiles[0], tiles[1], tiles[2], turned[2]),
                (
                    jnp.where(left, turned[2], turned[3]),
                    jnp.where(left, turned[3], turned[4]),
                    turned[4],
                    tiles[4],
                ),
            )
        ):
            three = jnp.where(left[:half], low[:half], high[half:])
            one, one_k = coded(one)
            two, two_k = coded(two)
            three, three_k = coded(three)
            g = order.index(2 * j + odd)
            out_ref[g, 0:WIDE, :] = one
            out_ref[g, WIDE : 2 * WIDE, :] = two
            out_ref[g, 2 * WIDE : 2 * WIDE + half, :] = three
            keys = jnp.where(row8 == 0, one_k, jnp.where(row8 == 1, two_k, three_k))
            out_ref[g, 2 * WIDE + half :, :] = keys.astype(I32).astype(I16)

    for j in range(pairs):
        pair(j)


def plane_sum_kernel(rows, order, q_ref, out_ref, table):
    half = WIDE // 2
    base = 2 * WIDE + half
    one = jnp.zeros((WIDE, LANES), F32)
    two = jnp.zeros((WIDE, LANES), F32)
    three = jnp.zeros((half, LANES), F32)
    for s in range(q_ref.shape[0]):
        keys = jnp.exp2(-q_ref[s, base:, :].astype(I32).astype(F32))
        one = one + q_ref[s, :WIDE, :].astype(I32).astype(F32) * keys[0:1]
        two = two + q_ref[s, WIDE : 2 * WIDE, :].astype(I32).astype(F32) * keys[1:2]
        three = three + q_ref[s, 2 * WIDE : base, :].astype(I32).astype(F32) * keys[2:3]
    table[0:LANES, :WIDE] = jnp.transpose(one)
    table[LANES : 2 * LANES, :WIDE] = jnp.transpose(two)
    three = jnp.transpose(three)
    mid = LANES // 2
    table[2 * LANES : 2 * LANES + mid, :WIDE] = jnp.concatenate(
        [three[:mid], three[mid:]], axis=1
    )
    for c in range(out_ref.shape[0]):
        block = table[rows * c : rows * (c + 1), :WIDE]
        k = exponent_of(jnp.max(jnp.abs(block), axis=(0, 1), keepdims=True))
        wide, rest = folded(jnp.round(block * jnp.exp2(k)))
        tail = out_ref.shape[1] - rows - rest.shape[0]
        piece = jnp.concatenate([wide, rest, jnp.broadcast_to(k, (tail, LANES))], axis=0)
        out_ref[order.index(c)] = piece.astype(I32).astype(I16)


def line_sum_kernel(q_ref, raw_ref, square_ref):
    deep = raw_ref.shape[0]
    raw = jnp.zeros(raw_ref.shape, F32)
    for s in range(q_ref.shape[0]):
        piece = q_ref[s].astype(I32).astype(F32)
        raw = raw + piece[:deep] * jnp.exp2(-piece[deep : deep + 1])
    raw_ref[...] = raw
    square = jnp.sum(raw * raw, axis=(0, 1), keepdims=True)
    square_ref[...] = jnp.broadcast_to(square[None], square_ref.shape)


def again_kernel(s_ref, out_ref):
    out_ref[...] = jnp.broadcast_to(jnp.sum(s_ref[...], axis=0, keepdims=True), out_ref.shape)


def clip_kernel(clip_norm, s_ref, raw_ref, out_ref):
    square = jnp.sum(s_ref[...], axis=0)[:, :1]
    scale = jnp.minimum(1.0, clip_norm / jnp.sqrt(square))
    out = raw_ref[...] * scale
    rows = out_ref.shape[0]
    step = rows // FOLD
    out_ref[:, 0, :LANES] = out[:rows]
    for g in range(FOLD):
        out_ref[step * g : step * (g + 1), 0, LANES:] = out[rows:, REST * g : REST * (g + 1)]


def call(kernel, *args, out, mib, scratch=(), name=None):
    vmem = pl.BlockSpec(memory_space=pltpu.VMEM)
    many = isinstance(out, list)
    return pl.pallas_call(
        kernel,
        out_shape=out,
        in_specs=[vmem] * len(args),
        out_specs=[vmem] * len(out) if many else vmem,
        scratch_shapes=list(scratch),
        compiler_params=pltpu.CompilerParams(vmem_limit_bytes=mib << 20),
        name=name,
    )(*args)


def shards(acts, cotangent, routes, router_weight):
    tokens, width = acts.shape[1:]
    rows, experts = router_weight.shape[1:]
    plane, line = size(PLANE), size(LINE)
    section = lax.axis_size("section")
    deep = rows * line
    fold_rows = rows + rows // FOLD
    fold_deep = deep + deep // FOLD
    like = jax.ShapeDtypeStruct

    weight = call(
        spread_kernel, router_weight[0], out=like((line, fold_rows, LANES), BF16), mib=2, name="spread"
    )
    weight = over_line(weight)
    weight = call(
        functools.partial(chunk_kernel, rows, line_order()),
        weight,
        out=like((plane, fold_deep, LANES), BF16),
        scratch=[pltpu.VMEM((deep, LANES), F32), pltpu.VMEM((deep // FOLD, LANES), F32)],
        mib=4, name="chunk",
    )
    weight = over_plane(weight)
    parts = call(
        functools.partial(layer_kernel, plane_order()),
        acts[0],
        weight,
        jnp.transpose(cotangent, (2, 0, 1)),
        jnp.transpose(routes, (2, 0, 1)),
        out=like((plane, fold_deep + 8, LANES), I16),
        scratch=[
            pltpu.VMEM((width, 2 * LANES), BF16),
            pltpu.VMEM((-(-tokens // LANES) * LANES, 2 * LANES), F32),
        ],
        mib=20, name="layer",
    )
    parts = over_plane(parts)
    parts = call(
        functools.partial(plane_sum_kernel, rows, line_order()),
        parts,
        out=like((line, 32, LANES), I16),
        scratch=[pltpu.VMEM((deep, 2 * LANES), F32)],
        mib=6, name="plane_sum",
    )
    parts = over_line(parts)
    raw, square = call(
        line_sum_kernel,
        parts,
        out=[like((fold_rows, LANES), F32), like((plane * section, 1, LANES), F32)],
        mib=2, name="line_sum",
    )
    square = over_plane_and_section(square)
    square = call(again_kernel, square, out=like((line, 1, LANES), F32), mib=1, name="again")
    square = over_line(square)
    clip_norm = 0.25 * math.sqrt(1.0 * section * width * experts)
    out = call(
        functools.partial(clip_kernel, clip_norm),
        square,
        raw,
        out=like((rows, 1, experts), F32),
        mib=1, name="clip",
    )
    return jnp.transpose(out, (1, 0, 2))


def solution(mesh):
    torus = Mesh(
        mesh.devices.reshape(4, 2, 2, 16, mesh.shape["section"]),
        ("batch_0", "batch_1", "seq_0", "seq_1", "section"),
    )
    placed = P("section", BATCH_SEQ, None)
    return jax.shard_map(
        shards,
        mesh=torus,
        in_specs=(placed, placed, placed, placed),
        out_specs=placed,
        check_vma=False,
    )
```
